128 devices in a mesh: rows: 4 (over z), cols: 8 (over x, core), slabs: 4 (over y).
Axes of the slice: x: 4, y: 4, z: 4, core: 2. Of those that a mesh axis runs over, the one named last changes fastest.
Arguments:
- pressure: float32 [512, 32, 128, 128], P('rows', 'cols', 'slabs'), may hold values from 0.5 to 2
- earlier: float32 [512, 32, 128, 128], P('rows', 'cols', 'slabs'), may hold values from 0.2 to 1.8
- speed_square: float32 [512, 32, 128, 128], P('rows', 'cols', 'slabs'), may hold values from 0.05 to 0.3
Outputs:
- scaled_field: float32 [512, 32, 128, 128], P('rows', 'cols', 'slabs')
- pressure_end: float32 [512, 32, 128, 128], P('rows', 'cols', 'slabs')
The draws below stay inside these ranges and needn't reach their ends.
All inputs are finite; a program needn't handle non-finite values.
Results may differ from the reference program's by a relative error of at most 0.00002.
Values sent between devices are 32-bit elements; how exact they have to be, the bound alone decides.
A program may use at most 128 MiB of HBM per device.

```python
import jax
import jax.numpy as jnp
from jax import lax

GRID_J = 512
GRID_I = 32
GRID_K = 128
MEMBERS = 128
STEPS = 3


def block_scale(key, extent, pieces, least, top_value):
    loudness, own = 1.0, jax.random.fold_in(key, 6)
    for position, blocks in pieces:
        heights = jnp.exp(jax.random.uniform(jax.random.fold_in(own, position), (blocks,), jnp.float32, least / len(pieces), top_value / len(pieces)))
        loudness = loudness * jnp.repeat(heights, extent[position] // blocks).reshape([-1 if axis == position else 1 for axis in range(len(extent))])
    return loudness


def setup_inputs(seed: int = 0) -> dict:
    streams_of = jax.random.split(jax.random.key(seed), 4)
    pressure = jnp.clip(0.5 + 1.5 * jax.random.uniform(streams_of[0], (GRID_J, GRID_I, GRID_K, MEMBERS), jnp.float32) ** block_scale(streams_of[0], (GRID_J, GRID_I, GRID_K, MEMBERS), ((0, 4), (1, 8), (2, 4)), -0.2, 0.2), 0.5, 2.0)
    earlier = jnp.clip(0.2 + 1.5999999 * jax.random.uniform(streams_of[1], (GRID_J, GRID_I, GRID_K, MEMBERS), jnp.float32) ** block_scale(streams_of[1], (GRID_J, GRID_I, GRID_K, MEMBERS), ((0, 4), (1, 8), (2, 4)), -0.2, 0.2), 0.2, 1.8)
    speed_square = jnp.clip(0.05 + 0.25 * jax.random.uniform(streams_of[2], (GRID_J, GRID_I, GRID_K, MEMBERS), jnp.float32) ** block_scale(streams_of[2], (GRID_J, GRID_I, GRID_K, MEMBERS), ((0, 4), (1, 8), (2, 4)), -0.2, 0.2), 0.05, 0.3)
    return dict(pressure=pressure, earlier=earlier, speed_square=speed_square)


def strip_edges(values, dims):
    for dim in dims:
        values = lax.slice_in_dim(values, 1, values.shape[dim] - 1, axis=dim)
    return values

def neighbour(values, dim, start, dims):
    others = [other for other in dims if other != dim]
    values = strip_edges(values, others)
    return lax.slice_in_dim(values, start, start + values.shape[dim] - 2, axis=dim)

def one_step(padded, before, speed_square):
    middle = strip_edges(padded, (0, 1, 2))
    lower = [neighbour(padded, dim, 0, (0, 1, 2)) for dim in (0, 1, 2)]
    upper = [neighbour(padded, dim, 2, (0, 1, 2)) for dim in (0, 1, 2)]
    spread = lower[0] + upper[0] + lower[1] + upper[1] + lower[2] + upper[2] - 6.0 * middle
    return 2.0 * middle - before + speed_square * spread

def reference(pressure, earlier, speed_square):
    for step in range(STEPS):
        later = one_step(jnp.pad(pressure, ((1, 1), (1, 1), (1, 1), (0, 0)), mode='wrap'), earlier, speed_square)
        earlier, pressure = (pressure, later)
    line_mean = lax.optimization_barrier(jnp.mean(pressure, axis=0, keepdims=True))
    centred = pressure - line_mean
    line_variance = lax.optimization_barrier(jnp.mean(centred * centred, axis=0, keepdims=True))
    scaled_field = centred * lax.rsqrt(line_variance + 0.0001)
    return (scaled_field, pressure)
```

```python
import functools

import jax
import jax.numpy as jnp
from jax import lax
from jax.experimental import pallas as pl
from jax.experimental.pallas import tpu as pltpu
from jax.sharding import PartitionSpec as P

STEPS = 3
MESH = pl.DeviceIdType.MESH
T = 8
ORDER = (3, 0, 1, 2)
GUESS = 1.0
UNROLL = 2


def exchange_kernel(
    p_hbm, e_hbm, s_hbm, out, norm,
    a, b, s, stats,
    load_sem, far_send, far_recv, near_send, near_recv,
    z_send, z_recv, y_send, y_recv, st_send, st_recv,
):
    nj, ni, nk, _ = out.shape
    tiles = nk // T
    zs, ys, xs = (lax.axis_size("rows"), lax.axis_size("slabs"), lax.axis_size("cols"))
    z, y, x = (lax.axis_index("rows"), lax.axis_index("slabs"), lax.axis_index("cols"))
    core = x % 2
    far_x = (x + 2 * core - 1 + xs) % xs
    near_x = x + 1 - 2 * core
    far, near = (1 + (ni - 1) * core, ni - (ni - 1) * core)
    far_halo, near_halo = ((ni + 1) * core, (ni + 1) * (1 - core))
    z_up, z_down = ((z + 1) % zs, (z + zs - 1) % zs)
    y_up, y_down = ((y + 1) % ys, (y + ys - 1) % ys)
    body = pl.ds(1, nj)
    levels = (a, b, a)

    def local(src, dst, n):
        return pltpu.make_async_copy(src, dst, load_sem.at[n])

    def rows_of(kc):
        return pl.ds(T + kc * T, T)

    loads = {}
    for n, kc in enumerate(ORDER):
        loads["far", kc] = local(
            p_hbm.at[:, far - 1, pl.ds(kc * T, T), :], a.at[body, far, rows_of(kc), :], n
        )
    n = tiles
    loads["near"] = local(p_hbm.at[:, near - 1], a.at[body, near, pl.ds(T, nk), :], n)
    loads["mid"] = local(p_hbm.at[:, pl.ds(1, ni - 2)], a.at[body, pl.ds(2, ni - 2), pl.ds(T, nk), :], n + 1)
    n += 2
    for kc in ORDER:
        loads["e", kc] = local(
            e_hbm.at[:, :, pl.ds(kc * T, T), :], b.at[body, pl.ds(1, ni), rows_of(kc), :], n
        )
        loads["s", kc] = local(
            s_hbm.at[:, :, pl.ds(kc * T, T), :], s.at[:, :, pl.ds(kc * T, T), :], n + 1
        )
        n += 2
    for copy in loads.values():
        copy.start()

    def remote(src, dst, send, recv, **where):
        return pltpu.make_async_remote_copy(
            src_ref=src, dst_ref=dst, send_sem=send, recv_sem=recv, device_id=where, device_id_type=MESH
        )

    def far_copy(t, kc):
        ref = levels[t]
        return remote(
            ref.at[body, far, rows_of(kc), :],
            ref.at[body, (ni + 1) * (1 - core), rows_of(kc), :],
            far_send.at[t, kc], far_recv.at[t, kc], cols=far_x,
        )

    def near_copy(t, kc):
        ref = levels[t]
        return remote(
            ref.at[body, near, rows_of(kc), :],
            ref.at[body, (ni + 1) * core, rows_of(kc), :],
            near_send.at[t, kc], near_recv.at[t, kc], cols=near_x,
        )

    def z_copies(t, kc):
        ref = levels[t]
        cells = pl.ds(1, ni)
        return (
            remote(
                ref.at[nj, cells, rows_of(kc), :], ref.at[0, cells, rows_of(kc), :],
                z_send.at[0, t, kc], z_recv.at[0, t, kc], rows=z_up,
            ),
            remote(
                ref.at[1, cells, rows_of(kc), :], ref.at[nj + 1, cells, rows_of(kc), :],
                z_send.at[1, t, kc], z_recv.at[1, t, kc], rows=z_down,
            ),
        )

    def y_copy(t, kc):
        ref = levels[t]
        cells = pl.ds(1, ni)
        if kc == 0:
            return remote(
                ref.at[body, cells, pl.ds(T, 1), :], ref.at[body, cells, pl.ds(T + nk, 1), :],
                y_send.at[0, t], y_recv.at[0, t], slabs=y_down,
            )
        return remote(
            ref.at[body, cells, pl.ds(T + nk - 1, 1), :], ref.at[body, cells, pl.ds(T - 1, 1), :],
            y_send.at[1, t], y_recv.at[1, t], slabs=y_up,
        )

    def faces(t, kc):
        yield far_copy(t, kc)
        yield near_copy(t, kc)
        yield from z_copies(t, kc)
        if kc in (0, tiles - 1):
            yield y_copy(t, kc)

    def wait_around(t, kc):
        near_copy(t, kc).wait_recv()
        for copy in z_copies(t, kc):
            copy.wait_recv()
        if kc == 0:
            y_copy(t, tiles - 1).wait_recv()
        if kc == tiles - 1:
            y_copy(t, 0).wait_recv()

    def stepped(now, before, j, i, kc):
        r = T + kc * T
        middle = now[j, i, pl.ds(r, T), :]
        total = now[j - 1, i, pl.ds(r, T), :] + now[j + 1, i, pl.ds(r, T), :]
        total = total + now[j, i - 1, pl.ds(r, T), :] + now[j, i + 1, pl.ds(r, T), :]
        total = total + now[j, i, pl.ds(r - 1, T), :] + now[j, i, pl.ds(r + 1, T), :]
        spread = total - 6.0 * middle
        earlier = before[j, i, pl.ds(r, T), :]
        return 2.0 * middle - earlier + s[j - 1, i - 1, pl.ds(kc * T, T), :] * spread

    barrier = pltpu.get_barrier_semaphore()
    peers = [dict(cols=far_x), dict(cols=near_x), dict(slabs=y_up), dict(slabs=y_down)]
    others = [dict(rows=(z + d) % zs) for d in range(1, zs)]
    for where in peers + others:
        pl.semaphore_signal(barrier, inc=1, device_id=where, device_id_type=MESH)
    pl.semaphore_wait(barrier, len(peers) + len(others))

    for kc in ORDER:
        loads["far", kc].wait()
        far_copy(0, kc).start()
    loads["near"].wait()
    for kc in ORDER:
        near_copy(0, kc).start()
    loads["mid"].wait()
    for kc in ORDER:
        for copy in z_copies(0, kc):
            copy.start()
    y_copy(0, tiles - 1).start()
    y_copy(0, 0).start()

    for t in range(STEPS - 1):
        now, before = (levels[t], levels[(t + 1) % 2])
        for kc in ORDER:
            if t == 0:
                loads["e", kc].wait()
                loads["s", kc].wait()
            else:
                for copy in faces(t - 1, kc):
                    copy.wait_send()
            wait_around(t, kc)
            far_copy(t, kc).wait_recv()

            @pl.loop(0, nj // UNROLL)
            def _(g, now=now, before=before, kc=kc):
                for u in range(UNROLL):
                    j = 1 + g * UNROLL + u
                    for i in range(1, ni + 1):
                        before[j, i, pl.ds(T + kc * T, T), :] = stepped(now, before, j, i, kc)

            for copy in faces(t + 1, kc):
                copy.start()

    t = STEPS - 1
    now, before = (levels[t], levels[t - 1])
    inner = [near] + [i for i in range(2, ni)]

    def last_step(planes, slots, kc):
        zero = jnp.zeros((T, out.shape[3]), jnp.float32)

        def loop(g, sums):
            sums = list(sums)
            for u in range(UNROLL):
                j = 1 + g * UNROLL + u
                for n, i in enumerate(planes):
                    value = stepped(now, before, j, i, kc)
                    out[j - 1, i - 1, pl.ds(kc * T, T), :] = value
                    moved = value - GUESS
                    sums[2 * n] = sums[2 * n] + moved
                    sums[2 * n + 1] = sums[2 * n + 1] + moved * moved
            return tuple(sums)

        sums = lax.fori_loop(0, nj // UNROLL, loop, (zero,) * (2 * len(planes)))
        for n, slot in enumerate(slots):
            stats[z, slot, 0, pl.ds(kc * T, T), :] = sums[2 * n]
            stats[z, slot, 1, pl.ds(kc * T, T), :] = sums[2 * n + 1]

    def inner_stats(n):
        part = stats.at[z, pl.ds(1, ni - 1)]
        return remote(part, part, st_send.at[n, tiles], st_recv.at[n, tiles], **others[n])

    def far_stats(n, kc):
        part = stats.at[z, 0, :, pl.ds(kc * T, T), :]
        return remote(part, part, st_send.at[n, kc], st_recv.at[n, kc], **others[n])

    def finish(i, slot, kc):
        totals = stats[0, slot, 0, pl.ds(kc * T, T), :]
        squares = stats[0, slot, 1, pl.ds(kc * T, T), :]
        for other in range(1, zs):
            totals = totals + stats[other, slot, 0, pl.ds(kc * T, T), :]
            squares = squares + stats[other, slot, 1, pl.ds(kc * T, T), :]
        count = nj * zs
        shift = totals * (1.0 / count)
        variance = squares * (1.0 / count) - shift * shift
        norm[0, i - 1, pl.ds(kc * T, T), :] = GUESS + shift
        norm[1, i - 1, pl.ds(kc * T, T), :] = lax.rsqrt(variance + 0.0001)

    for kc in ORDER:
        wait_around(t, kc)
        last_step(inner, range(1, ni), kc)
    for n in range(len(others)):
        inner_stats(n).start()
    for kc in ORDER:
        far_copy(t, kc).wait_recv()
        last_step([far], [0], kc)
        for n in range(len(others)):
            far_stats(n, kc).start()
    for n in range(len(others)):
        inner_stats(n).wait_recv()
    for n, i in enumerate(inner):
        for kc in ORDER:
            finish(i, n + 1, kc)
    for kc in ORDER:
        for n in range(len(others)):
            far_stats(n, kc).wait_recv()
        finish(far, 0, kc)

    for last in (t - 1, t):
        for kc in ORDER:
            for copy in faces(last, kc):
                copy.wait_send()
    for n in range(len(others)):
        inner_stats(n).wait_send()
        for kc in ORDER:
            far_stats(n, kc).wait_send()


def write_kernel(p, norm, scaled_hbm, end_hbm, scaled, sems):
    nj, ni, nk, _ = p.shape
    pieces = sems.shape[0] - 1
    step = nj // pieces
    end = pltpu.make_async_copy(p, end_hbm, sems.at[pieces])
    end.start()

    def copy(n):
        part = pl.ds(n * step, step)
        return pltpu.make_async_copy(scaled.at[part], scaled_hbm.at[part], sems.at[n])

    for n in range(pieces):
        for i in range(ni):
            for kc in range(nk // T):
                rows = pl.ds(kc * T, T)
                mean, scale = (norm[0, i, rows, :], norm[1, i, rows, :])

                @pl.loop(n * step, (n + 1) * step, unroll=8)
                def _(j):
                    scaled[j, i, rows, :] = (p[j, i, rows, :] - mean) * scale

        copy(n).start()
    for n in range(pieces):
        copy(n).wait()
    end.wait()


def shards(pressure, earlier, speed_square):
    nj, ni, nk, members = pressure.shape
    tiles = nk // T
    zs = lax.axis_size("rows")
    whole = pl.BlockSpec(memory_space=pl.ANY)
    vmem = pl.BlockSpec(memory_space=pltpu.VMEM)
    f32 = jnp.float32
    dma = pltpu.SemaphoreType.DMA
    p, norm = pl.pallas_call(
        exchange_kernel,
        out_shape=(
            pltpu.VMEM((nj, ni, nk, members), f32),
            pltpu.VMEM((2, ni, nk, members), f32),
        ),
        in_specs=[whole] * 3,
        out_specs=(vmem, vmem),
        scratch_shapes=[
            pltpu.VMEM((nj + 2, ni + 2, nk + 2 * T, members), f32),
            pltpu.VMEM((nj + 2, ni + 2, nk + 2 * T, members), f32),
            pltpu.VMEM((nj, ni, nk, members), f32),
            pltpu.VMEM((zs, ni, 2, nk, members), f32),
            dma((3 * tiles + 2,)),
            dma((STEPS, tiles)), dma((STEPS, tiles)),
            dma((STEPS, tiles)), dma((STEPS, tiles)),
            dma((2, STEPS, tiles)), dma((2, STEPS, tiles)),
            dma((2, STEPS)), dma((2, STEPS)),
            dma((zs - 1, tiles + 1)), dma((zs - 1, tiles + 1)),
        ],
        compiler_params=pltpu.CompilerParams(
            collective_id=0, has_side_effects=True, vmem_limit_bytes=50 << 20
        ),
        name="leapfrog",
    )(pressure, earlier, speed_square)
    pieces = 8
    return pl.pallas_call(
        write_kernel,
        out_shape=(jax.ShapeDtypeStruct(p.shape, f32),) * 2,
        in_specs=[vmem, vmem],
        out_specs=(whole, whole),
        scratch_shapes=[pltpu.VMEM(p.shape, f32), dma((pieces + 1,))],
        compiler_params=pltpu.CompilerParams(vmem_limit_bytes=20 << 20),
        name="centre_and_scale",
    )(p, norm)


def solution(mesh):
    spec = P("rows", "cols", "slabs", None)
    return jax.shard_map(shards, mesh=mesh, in_specs=(spec,) * 3, out_specs=(spec,) * 2, check_vma=False)
```

```python
import functools

import jax
import jax.numpy as jnp
from jax import lax
from jax.experimental import pallas as pl
from jax.experimental.pallas import tpu as pltpu
from jax.sharding import PartitionSpec as P

STEPS = 3
MESH = pl.DeviceIdType.MESH
T = 8
ORDER = (3, 0, 1, 2)
TAIL = (2, 4, 8, 8)
GUESS = 1.0
UNROLL = 2


def exchange_kernel(
    p_hbm, e_hbm, s_hbm, out, norm,
    a, b, s, stats,
    load_sem, far_send, far_recv, near_send, near_recv,
    z_send, z_recv, y_send, y_recv, st_send, st_recv,
):
    nj, ni, nk, _ = out.shape
    tiles = nk // T
    zs, ys, xs = (lax.axis_size("rows"), lax.axis_size("slabs"), lax.axis_size("cols"))
    z, y, x = (lax.axis_index("rows"), lax.axis_index("slabs"), lax.axis_index("cols"))
    core = x % 2
    far_x = (x + 2 * core - 1 + xs) % xs
    near_x = x + 1 - 2 * core
    far, near = (1 + (ni - 1) * core, ni - (ni - 1) * core)
    far_halo, near_halo = ((ni + 1) * core, (ni + 1) * (1 - core))
    z_up, z_down = ((z + 1) % zs, (z + zs - 1) % zs)
    y_up, y_down = ((y + 1) % ys, (y + ys - 1) % ys)
    body = pl.ds(1, nj)
    levels = (a, b, a)

    def local(src, dst, n):
        return pltpu.make_async_copy(src, dst, load_sem.at[n])

    def rows_of(kc):
        return pl.ds(T + kc * T, T)

    loads = {}
    for n, kc in enumerate(ORDER):
        loads["far", kc] = local(
            p_hbm.at[:, far - 1, pl.ds(kc * T, T), :], a.at[body, far, rows_of(kc), :], n
        )
    n = tiles
    loads["near"] = local(p_hbm.at[:, near - 1], a.at[body, near, pl.ds(T, nk), :], n)
    loads["mid"] = local(p_hbm.at[:, pl.ds(1, ni - 2)], a.at[body, pl.ds(2, ni - 2), pl.ds(T, nk), :], n + 1)
    n += 2
    for kc in ORDER:
        loads["e", kc] = local(
            e_hbm.at[:, :, pl.ds(kc * T, T), :], b.at[body, pl.ds(1, ni), rows_of(kc), :], n
        )
        loads["s", kc] = local(
            s_hbm.at[:, :, pl.ds(kc * T, T), :], s.at[:, :, pl.ds(kc * T, T), :], n + 1
        )
        n += 2
    for copy in loads.values():
        copy.start()

    def remote(src, dst, send, recv, **where):
        return pltpu.make_async_remote_copy(
            src_ref=src, dst_ref=dst, send_sem=send, recv_sem=recv, device_id=where, device_id_type=MESH
        )

    def far_piece(t, kc, n, start, size):
        ref = levels[t]
        part = pl.ds(1 + start, size)
        return remote(
            ref.at[part, far, rows_of(kc), :],
            ref.at[part, (ni + 1) * (1 - core), rows_of(kc), :],
            far_send.at[t, kc + n], far_recv.at[t, kc + n], cols=far_x,
        )

    def pieces_of(t, kc):
        if t < STEPS - 1 or kc != ORDER[-1]:
            return [(kc, 0, 0, nj)]
        starts = [0]
        for part in TAIL:
            starts.append(starts[-1] + nj // part)
        ids = [0] + [tiles - kc + n for n in range(len(TAIL) - 1)]
        return [(kc, n, a0, a1 - a0) for n, a0, a1 in zip(ids, starts, starts[1:])]

    def far_copies(t, kc):
        return [far_piece(t, *piece) for piece in pieces_of(t, kc)]

    def near_copy(t, kc):
        ref = levels[t]
        return remote(
            ref.at[body, near, rows_of(kc), :],
            ref.at[body, (ni + 1) * core, rows_of(kc), :],
            near_send.at[t, kc], near_recv.at[t, kc], cols=near_x,
        )

    def z_copies(t, kc):
        ref = levels[t]
        cells = pl.ds(1, ni)
        return (
            remote(
                ref.at[nj, cells, rows_of(kc), :], ref.at[0, cells, rows_of(kc), :],
                z_send.at[0, t, kc], z_recv.at[0, t, kc], rows=z_up,
            ),
            remote(
                ref.at[1, cells, rows_of(kc), :], ref.at[nj + 1, cells, rows_of(kc), :],
                z_send.at[1, t, kc], z_recv.at[1, t, kc], rows=z_down,
            ),
        )

    def y_copy(t, kc):
        ref = levels[t]
        cells = pl.ds(1, ni)
        if kc == 0:
            return remote(
                ref.at[body, cells, pl.ds(T, 1), :], ref.at[body, cells, pl.ds(T + nk, 1), :],
                y_send.at[0, t], y_recv.at[0, t], slabs=y_down,
            )
        return remote(
            ref.at[body, cells, pl.ds(T + nk - 1, 1), :], ref.at[body, cells, pl.ds(T - 1, 1), :],
            y_send.at[1, t], y_recv.at[1, t], slabs=y_up,
        )

    def faces(t, kc):
        yield from far_copies(t, kc)
        yield near_copy(t, kc)
        yield from z_copies(t, kc)
        if kc in (0, tiles - 1):
            yield y_copy(t, kc)

    def wait_around(t, kc):
        near_copy(t, kc).wait_recv()
        for copy in z_copies(t, kc):
            copy.wait_recv()
        if kc == 0:
            y_copy(t, tiles - 1).wait_recv()
        if kc == tiles - 1:
            y_copy(t, 0).wait_recv()

    def stepped(now, before, j, i, kc):
        r = T + kc * T
        middle = now[j, i, pl.ds(r, T), :]
        total = now[j - 1, i, pl.ds(r, T), :] + now[j + 1, i, pl.ds(r, T), :]
        total = total + now[j, i - 1, pl.ds(r, T), :] + now[j, i + 1, pl.ds(r, T), :]
        total = total + now[j, i, pl.ds(r - 1, T), :] + now[j, i, pl.ds(r + 1, T), :]
        spread = total - 6.0 * middle
        earlier = before[j, i, pl.ds(r, T), :]
        return 2.0 * middle - earlier + s[j - 1, i - 1, pl.ds(kc * T, T), :] * spread

    barrier = pltpu.get_barrier_semaphore()
    peers = [dict(cols=far_x), dict(cols=near_x), dict(slabs=y_up), dict(slabs=y_down)]
    others = [dict(rows=(z + d) % zs) for d in (2, 1, 3)]
    for where in peers + others:
        pl.semaphore_signal(barrier, inc=1, device_id=where, device_id_type=MESH)
    pl.semaphore_wait(barrier, len(peers) + len(others))

    for kc in ORDER:
        loads["far", kc].wait()
        for copy in far_copies(0, kc):
            copy.start()
    loads["near"].wait()
    for kc in ORDER:
        near_copy(0, kc).start()
    loads["mid"].wait()
    for kc in ORDER:
        for copy in z_copies(0, kc):
            copy.start()
    y_copy(0, tiles - 1).start()
    y_copy(0, 0).start()

    for t in range(STEPS - 1):
        now, before = (levels[t], levels[(t + 1) % 2])
        for kc in ORDER:
            if t == 0:
                loads["e", kc].wait()
                loads["s", kc].wait()
            else:
                for copy in faces(t - 1, kc):
                    copy.wait_send()
            wait_around(t, kc)
            for copy in far_copies(t, kc):
                copy.wait_recv()

            @pl.loop(0, nj // UNROLL)
            def _(g, now=now, before=before, kc=kc):
                for u in range(UNROLL):
                    j = 1 + g * UNROLL + u
                    for i in range(1, ni + 1):
                        before[j, i, pl.ds(T + kc * T, T), :] = stepped(now, before, j, i, kc)

            for copy in faces(t + 1, kc):
                copy.start()

    t = STEPS - 1
    now, before = (levels[t], levels[t - 1])
    inner = [near] + [i for i in range(2, ni)]

    def last_step(planes, kc, start, size, sums):
        def loop(g, sums):
            sums = list(sums)
            for u in range(UNROLL):
                j = 1 + start + g * UNROLL + u
                for n, i in enumerate(planes):
                    value = stepped(now, before, j, i, kc)
                    out[j - 1, i - 1, pl.ds(kc * T, T), :] = value
                    moved = value - GUESS
                    sums[2 * n] = sums[2 * n] + moved
                    sums[2 * n + 1] = sums[2 * n + 1] + moved * moved
            return tuple(sums)

        if sums is None:
            sums = (jnp.zeros((T, out.shape[3]), jnp.float32),) * (2 * len(planes))
        return lax.fori_loop(0, size // UNROLL, loop, sums)

    def put_sums(slots, kc, sums):
        for n, slot in enumerate(slots):
            stats[z, slot, 0, pl.ds(kc * T, T), :] = sums[2 * n]
            stats[z, slot, 1, pl.ds(kc * T, T), :] = sums[2 * n + 1]

    def inner_stats(n):
        part = stats.at[z, pl.ds(1, ni - 1)]
        return remote(part, part, st_send.at[n, tiles], st_recv.at[n, tiles], **others[n])

    def far_stats(n, kc):
        part = stats.at[z, 0, :, pl.ds(kc * T, T), :]
        return remote(part, part, st_send.at[n, kc], st_recv.at[n, kc], **others[n])

    def finish(i, slot, kc):
        totals = stats[0, slot, 0, pl.ds(kc * T, T), :]
        squares = stats[0, slot, 1, pl.ds(kc * T, T), :]
        for other in range(1, zs):
            totals = totals + stats[other, slot, 0, pl.ds(kc * T, T), :]
            squares = squares + stats[other, slot, 1, pl.ds(kc * T, T), :]
        count = nj * zs
        shift = totals * (1.0 / count)
        variance = squares * (1.0 / count) - shift * shift
        norm[0, i - 1, pl.ds(kc * T, T), :] = GUESS + shift
        norm[1, i - 1, pl.ds(kc * T, T), :] = lax.rsqrt(variance + 0.0001)

    for kc in ORDER:
        wait_around(t, kc)
        put_sums(range(1, ni), kc, last_step(inner, kc, 0, nj, None))
    for n in range(len(others)):
        inner_stats(n).start()
    for kc in ORDER:
        for copy in faces(t - 1, kc):
            copy.wait_send()

    def finish_far(kc):
        for n in range(len(others)):
            far_stats(n, kc).wait_recv()
        finish(far, 0, kc)

    for kc in ORDER:
        sums = None
        for piece, copy in zip(pieces_of(t, kc), far_copies(t, kc)):
            copy.wait_recv()
            sums = last_step([far], kc, piece[2], piece[3], sums)
        put_sums([0], kc, sums)
        for n in range(len(others)):
            far_stats(n, kc).start()
        if kc == ORDER[1]:
            for n in range(len(others)):
                inner_stats(n).wait_recv()
            for n, i in enumerate(inner):
                for tile in ORDER:
                    finish(i, n + 1, tile)
            for tile in ORDER:
                near_copy(t, tile).wait_send()
                for copy in z_copies(t, tile):
                    copy.wait_send()
            for tile in (0, tiles - 1):
                y_copy(t, tile).wait_send()
            for n in range(len(others)):
                inner_stats(n).wait_send()
        if kc == ORDER[2]:
            for tile in ORDER[:2]:
                finish_far(tile)
                for copy in far_copies(t, tile):
                    copy.wait_send()
                for n in range(len(others)):
                    far_stats(n, tile).wait_send()
    for tile in ORDER[2:]:
        finish_far(tile)
    for tile in ORDER[2:]:
        for copy in far_copies(t, tile):
            copy.wait_send()
        for n in range(len(others)):
            far_stats(n, tile).wait_send()


def write_kernel(p, norm, scaled_hbm, end_hbm, scaled, sems):
    nj, ni, nk, _ = p.shape
    pieces = sems.shape[1]
    step = nj // pieces

    def end(n):
        part = pl.ds(n * step, step)
        return pltpu.make_async_copy(p.at[part], end_hbm.at[part], sems.at[1, n])

    for n in range(pieces):
        end(n).start()

    def copy(n):
        part = pl.ds(n * step, step)
        return pltpu.make_async_copy(scaled.at[part], scaled_hbm.at[part], sems.at[0, n])

    for n in range(pieces):
        for i in range(ni):
            for kc in range(nk // T):
                rows = pl.ds(kc * T, T)
                mean, scale = (norm[0, i, rows, :], norm[1, i, rows, :])

                @pl.loop(n * step, (n + 1) * step, unroll=8)
                def _(j):
                    scaled[j, i, rows, :] = (p[j, i, rows, :] - mean) * scale

        copy(n).start()
    for n in range(pieces):
        copy(n).wait()
        end(n).wait()


def shards(pressure, earlier, speed_square):
    nj, ni, nk, members = pressure.shape
    tiles = nk // T
    zs = lax.axis_size("rows")
    whole = pl.BlockSpec(memory_space=pl.ANY)
    vmem = pl.BlockSpec(memory_space=pltpu.VMEM)
    f32 = jnp.float32
    dma = pltpu.SemaphoreType.DMA
    p, norm = pl.pallas_call(
        exchange_kernel,
        out_shape=(
            pltpu.VMEM((nj, ni, nk, members), f32),
            pltpu.VMEM((2, ni, nk, members), f32),
        ),
        in_specs=[whole] * 3,
        out_specs=(vmem, vmem),
        scratch_shapes=[
            pltpu.VMEM((nj + 2, ni + 2, nk + 2 * T, members), f32),
            pltpu.VMEM((nj + 2, ni + 2, nk + 2 * T, members), f32),
            pltpu.VMEM((nj, ni, nk, members), f32),
            pltpu.VMEM((zs, ni, 2, nk, members), f32),
            dma((3 * tiles + 2,)),
            dma((STEPS, tiles + len(TAIL) - 1)), dma((STEPS, tiles + len(TAIL) - 1)),
            dma((STEPS, tiles)), dma((STEPS, tiles)),
            dma((2, STEPS, tiles)), dma((2, STEPS, tiles)),
            dma((2, STEPS)), dma((2, STEPS)),
            dma((zs - 1, tiles + 1)), dma((zs - 1, tiles + 1)),
        ],
        compiler_params=pltpu.CompilerParams(
            collective_id=0, has_side_effects=True, vmem_limit_bytes=50 << 20
        ),
        name="leapfrog",
    )(pressure, earlier, speed_square)
    pieces = 8
    return pl.pallas_call(
        write_kernel,
        out_shape=(jax.ShapeDtypeStruct(p.shape, f32),) * 2,
        in_specs=[vmem, vmem],
        out_specs=(whole, whole),
        scratch_shapes=[pltpu.VMEM(p.shape, f32), dma((2, pieces))],
        compiler_params=pltpu.CompilerParams(vmem_limit_bytes=20 << 20),
        name="centre_and_scale",
    )(p, norm)


def solution(mesh):
    spec = P("rows", "cols", "slabs", None)
    return jax.shard_map(shards, mesh=mesh, in_specs=(spec,) * 3, out_specs=(spec,) * 2, check_vma=False)
```

```python
import functools

import jax
import jax.numpy as jnp
from jax import lax
from jax.experimental import pallas as pl
from jax.experimental.pallas import tpu as pltpu
from jax.sharding import PartitionSpec as P

STEPS = 3
MESH = pl.DeviceIdType.MESH
T = 8
ORDER = (3, 0, 1, 2)
TAIL = (2, 4, 8, 8)
GUESS = 1.0
UNROLL = 2


def exchange_kernel(
    p_hbm, e_hbm, s_hbm, out, norm,
    a, b, s, stats,
    load_sem, face_send, face_recv, far_recv, sums_send, sums_recv,
):
    nj, ni, nk, _ = out.shape
    tiles = nk // T
    zs, ys, xs = (lax.axis_size("rows"), lax.axis_size("slabs"), lax.axis_size("cols"))
    z, y, x = (lax.axis_index("rows"), lax.axis_index("slabs"), lax.axis_index("cols"))
    core = x % 2
    far_x = (x + 2 * core - 1 + xs) % xs
    near_x = x + 1 - 2 * core
    far, near = (1 + (ni - 1) * core, ni - (ni - 1) * core)
    far_halo, near_halo = ((ni + 1) * core, (ni + 1) * (1 - core))
    z_up, z_down = ((z + 1) % zs, (z + zs - 1) % zs)
    y_up, y_down = ((y + 1) % ys, (y + ys - 1) % ys)
    body = pl.ds(1, nj)
    levels = (a, b, a)

    def local(src, dst, n):
        return pltpu.make_async_copy(src, dst, load_sem.at[n])

    def wait_for(tiles_landed, sem):
        depth = tiles if tiles_landed % (ni * tiles) == 0 else 1
        part = (pl.ds(0, tiles_landed // (ni * depth)), pl.ds(0, ni), pl.ds(0, depth * T))
        pltpu.make_async_copy(p_hbm.at[part], s.at[part], sem).wait()

    plane = nj * tiles
    near_tiles, y_tiles, z_tiles = (nj, nj * ni // T, ni)

    def rows_of(kc):
        return pl.ds(T + kc * T, T)

    loads = []
    for kc in ORDER:
        loads.append(local(
            p_hbm.at[:, far - 1, pl.ds(kc * T, T), :], a.at[body, far, rows_of(kc), :], 0
        ))
    loads.append(local(p_hbm.at[:, near - 1], a.at[body, near, pl.ds(T, nk), :], 1))
    loads.append(local(
        p_hbm.at[:, pl.ds(1, ni - 2)], a.at[body, pl.ds(2, ni - 2), pl.ds(T, nk), :], 1
    ))
    for n, kc in enumerate(ORDER):
        loads.append(local(
            e_hbm.at[:, :, pl.ds(kc * T, T), :], b.at[body, pl.ds(1, ni), rows_of(kc), :], n + 2
        ))
        loads.append(local(
            s_hbm.at[:, :, pl.ds(kc * T, T), :], s.at[:, :, pl.ds(kc * T, T), :], n + 2
        ))
    for copy in loads:
        copy.start()

    def remote(src, dst, send, recv, **where):
        return pltpu.make_async_remote_copy(
            src_ref=src, dst_ref=dst, send_sem=send, recv_sem=recv, device_id=where, device_id_type=MESH
        )

    def far_piece(t, kc, n, start, size):
        ref = levels[t]
        part = pl.ds(1 + start, size)
        return remote(
            ref.at[part, far, rows_of(kc), :],
            ref.at[part, (ni + 1) * (1 - core), rows_of(kc), :],
            face_send.at[t], far_recv.at[kc + n] if t == STEPS - 1 else face_recv.at[t, kc], cols=far_x,
        )

    def pieces_of(t, kc):
        if t < STEPS - 1 or kc != ORDER[-1]:
            return [(kc, 0, 0, nj)]
        starts = [0]
        for part in TAIL:
            starts.append(starts[-1] + nj // part)
        ids = [0] + [tiles - kc + n for n in range(len(TAIL) - 1)]
        return [(kc, n, a0, a1 - a0) for n, a0, a1 in zip(ids, starts, starts[1:])]

    def far_copies(t, kc):
        return [far_piece(t, *piece) for piece in pieces_of(t, kc)]

    def near_copy(t, kc):
        ref = levels[t]
        return remote(
            ref.at[body, near, rows_of(kc), :],
            ref.at[body, (ni + 1) * core, rows_of(kc), :],
            face_send.at[t], face_recv.at[t, kc], cols=near_x,
        )

    def z_copies(t, kc):
        ref = levels[t]
        cells = pl.ds(1, ni)
        return (
            remote(
                ref.at[nj, cells, rows_of(kc), :], ref.at[0, cells, rows_of(kc), :],
                face_send.at[t], face_recv.at[t, kc], rows=z_up,
            ),
            remote(
                ref.at[1, cells, rows_of(kc), :], ref.at[nj + 1, cells, rows_of(kc), :],
                face_send.at[t], face_recv.at[t, kc], rows=z_down,
            ),
        )

    def y_copy(t, kc):
        ref = levels[t]
        cells = pl.ds(1, ni)
        if kc == 0:
            return remote(
                ref.at[body, cells, pl.ds(T, 1), :], ref.at[body, cells, pl.ds(T + nk, 1), :],
                face_send.at[t], face_recv.at[t, tiles - 1], slabs=y_down,
            )
        return remote(
            ref.at[body, cells, pl.ds(T + nk - 1, 1), :], ref.at[body, cells, pl.ds(T - 1, 1), :],
            face_send.at[t], face_recv.at[t, 0], slabs=y_up,
        )

    def faces(t, kc):
        yield from far_copies(t, kc)
        yield near_copy(t, kc)
        yield from z_copies(t, kc)
        if kc in (0, tiles - 1):
            yield y_copy(t, kc)

    def wait_faces(t, kc):
        landed = near_tiles + 2 * z_tiles
        if t < STEPS - 1:
            landed += near_tiles
        if kc in (0, tiles - 1):
            landed += y_tiles
        wait_for(landed, face_recv.at[t, kc])

    def wait_faces_sent(t):
        wait_for(2 * plane + 2 * z_tiles * tiles + 2 * y_tiles, face_send.at[t])

    def stepped(now, before, j, i, kc):
        r = T + kc * T
        middle = now[j, i, pl.ds(r, T), :]
        total = now[j - 1, i, pl.ds(r, T), :] + now[j + 1, i, pl.ds(r, T), :]
        total = total + now[j, i - 1, pl.ds(r, T), :] + now[j, i + 1, pl.ds(r, T), :]
        total = total + now[j, i, pl.ds(r - 1, T), :] + now[j, i, pl.ds(r + 1, T), :]
        spread = total - 6.0 * middle
        earlier = before[j, i, pl.ds(r, T), :]
        return 2.0 * middle - earlier + s[j - 1, i - 1, pl.ds(kc * T, T), :] * spread

    barrier = pltpu.get_barrier_semaphore()
    peers = [dict(cols=far_x), dict(cols=near_x), dict(slabs=y_up), dict(slabs=y_down)]
    others = [dict(rows=(z + d) % zs) for d in (2, 1, 3)]
    for where in peers + others:
        pl.semaphore_signal(barrier, inc=1, device_id=where, device_id_type=MESH)
    pl.semaphore_wait(barrier, len(peers) + len(others))

    wait_for(plane, load_sem.at[0])
    for kc in ORDER:
        for copy in far_copies(0, kc):
            copy.start()
    wait_for((ni - 1) * plane, load_sem.at[1])
    for kc in ORDER:
        near_copy(0, kc).start()
    for kc in ORDER:
        for copy in z_copies(0, kc):
            copy.start()
    y_copy(0, tiles - 1).start()
    y_copy(0, 0).start()

    for t in range(STEPS - 1):
        now, before = (levels[t], levels[(t + 1) % 2])
        if t > 0:
            wait_faces_sent(t - 1)
        for n, kc in enumerate(ORDER):
            if t == 0:
                wait_for(2 * ni * nj, load_sem.at[n + 2])
            wait_faces(t, kc)

            @pl.loop(0, nj // UNROLL)
            def _(g, now=now, before=before, kc=kc):
                for u in range(UNROLL):
                    j = 1 + g * UNROLL + u
                    for i in range(1, ni + 1):
                        before[j, i, pl.ds(T + kc * T, T), :] = stepped(now, before, j, i, kc)

            for copy in faces(t + 1, kc):
                copy.start()

    t = STEPS - 1
    now, before = (levels[t], levels[t - 1])
    inner = [near] + [i for i in range(2, ni)]

    def last_step(planes, kc, start, size, sums):
        def loop(g, sums):
            sums = list(sums)
            for u in range(UNROLL):
                j = 1 + start + g * UNROLL + u
                for n, i in enumerate(planes):
                    value = stepped(now, before, j, i, kc)
                    out[j - 1, i - 1, pl.ds(kc * T, T), :] = value
                    moved = value - GUESS
                    sums[2 * n] = sums[2 * n] + moved
                    sums[2 * n + 1] = sums[2 * n + 1] + moved * moved
            return tuple(sums)

        if sums is None:
            sums = (jnp.zeros((T, out.shape[3]), jnp.float32),) * (2 * len(planes))
        return lax.fori_loop(0, size // UNROLL, loop, sums)

    def put_sums(slots, kc, sums):
        for n, slot in enumerate(slots):
            stats[z, slot, 0, pl.ds(kc * T, T), :] = sums[2 * n]
            stats[z, slot, 1, pl.ds(kc * T, T), :] = sums[2 * n + 1]

    def send_sums(part, group):
        for where in others:
            remote(part, part, sums_send, sums_recv.at[group], **where).start()

    def finish(i, slot, kc):
        totals = stats[0, slot, 0, pl.ds(kc * T, T), :]
        squares = stats[0, slot, 1, pl.ds(kc * T, T), :]
        for other in range(1, zs):
            totals = totals + stats[other, slot, 0, pl.ds(kc * T, T), :]
            squares = squares + stats[other, slot, 1, pl.ds(kc * T, T), :]
        count = nj * zs
        shift = totals * (1.0 / count)
        variance = squares * (1.0 / count) - shift * shift
        norm[0, i - 1, pl.ds(kc * T, T), :] = GUESS + shift
        norm[1, i - 1, pl.ds(kc * T, T), :] = lax.rsqrt(variance + 0.0001)

    for kc in ORDER:
        wait_faces(t, kc)
        put_sums(range(1, ni), kc, last_step(inner, kc, 0, nj, None))
    send_sums(stats.at[z, pl.ds(1, ni - 1)], 0)
    wait_faces_sent(t - 1)
    peers_sums = 2 * len(others)
    for n, kc in enumerate(ORDER):
        sums = None
        for piece, copy in zip(pieces_of(t, kc), far_copies(t, kc)):
            copy.wait_recv()
            sums = last_step([far], kc, piece[2], piece[3], sums)
        put_sums([0], kc, sums)
        send_sums(stats.at[z, 0, :, pl.ds(kc * T, T), :], n // 2)
        if n == 2:
            wait_for(peers_sums * ((ni - 1) * tiles + 2), sums_recv.at[0])
            for slot, i in enumerate(inner):
                for tile in ORDER:
                    finish(i, slot + 1, tile)
            for tile in ORDER[:2]:
                finish(far, 0, tile)
    wait_for(peers_sums * 2, sums_recv.at[1])
    for tile in ORDER[2:]:
        finish(far, 0, tile)
    wait_faces_sent(t)
    wait_for(peers_sums * ni * tiles, sums_send)


def write_kernel(p, norm, scaled_hbm, end_hbm, scaled, sems):
    nj, ni, nk, _ = p.shape
    pieces = sems.shape[1]
    step = nj // pieces

    def end(n):
        part = pl.ds(n * step, step)
        return pltpu.make_async_copy(p.at[part], end_hbm.at[part], sems.at[1, n])

    for n in range(pieces):
        end(n).start()

    def copy(n):
        part = pl.ds(n * step, step)
        return pltpu.make_async_copy(scaled.at[part], scaled_hbm.at[part], sems.at[0, n])

    for n in range(pieces):
        for i in range(ni):
            for kc in range(nk // T):
                rows = pl.ds(kc * T, T)
                mean, scale = (norm[0, i, rows, :], norm[1, i, rows, :])

                @pl.loop(n * step, (n + 1) * step, unroll=8)
                def _(j):
                    scaled[j, i, rows, :] = (p[j, i, rows, :] - mean) * scale

        copy(n).start()
    for n in range(pieces):
        copy(n).wait()
        end(n).wait()


def shards(pressure, earlier, speed_square):
    nj, ni, nk, members = pressure.shape
    tiles = nk // T
    zs = lax.axis_size("rows")
    whole = pl.BlockSpec(memory_space=pl.ANY)
    vmem = pl.BlockSpec(memory_space=pltpu.VMEM)
    f32 = jnp.float32
    dma = pltpu.SemaphoreType.DMA
    p, norm = pl.pallas_call(
        exchange_kernel,
        out_shape=(
            pltpu.VMEM((nj, ni, nk, members), f32),
            pltpu.VMEM((2, ni, nk, members), f32),
        ),
        in_specs=[whole] * 3,
        out_specs=(vmem, vmem),
        scratch_shapes=[
            pltpu.VMEM((nj + 2, ni + 2, nk + 2 * T, members), f32),
            pltpu.VMEM((nj + 2, ni + 2, nk + 2 * T, members), f32),
            pltpu.VMEM((nj, ni, nk, members), f32),
            pltpu.VMEM((zs, ni, 2, nk, members), f32),
            dma((tiles + 2,)),
            dma((STEPS,)), dma((STEPS, tiles)), dma((tiles + len(TAIL) - 1,)),
            dma, dma((2,)),
        ],
        compiler_params=pltpu.CompilerParams(
            collective_id=0, has_side_effects=True, vmem_limit_bytes=50 << 20
        ),
        name="leapfrog",
    )(pressure, earlier, speed_square)
    pieces = 8
    return pl.pallas_call(
        write_kernel,
        out_shape=(jax.ShapeDtypeStruct(p.shape, f32),) * 2,
        in_specs=[vmem, vmem],
        out_specs=(whole, whole),
        scratch_shapes=[pltpu.VMEM(p.shape, f32), dma((2, pieces))],
        compiler_params=pltpu.CompilerParams(vmem_limit_bytes=20 << 20),
        name="centre_and_scale",
    )(p, norm)


def solution(mesh):
    spec = P("rows", "cols", "slabs", None)
    return jax.shard_map(shards, mesh=mesh, in_specs=(spec,) * 3, out_specs=(spec,) * 2, check_vma=False)
```

```python
import functools

import jax
import jax.numpy as jnp
from jax import lax
from jax.experimental import pallas as pl
from jax.experimental.pallas import tpu as pltpu
from jax.sharding import PartitionSpec as P

STEPS = 3
MESH = pl.DeviceIdType.MESH
T = 8
ORDER = (3, 0, 1, 2)
TAIL = (2, 4, 8, 8)
GUESS = 1.0
UNROLL = 2


def exchange_kernel(
    p_hbm, e_hbm, s_hbm, out, norm,
    a, b, s, stats,
    load_sem, face_send, face_recv, far_recv, sums_send, sums_recv,
):
    nj, ni, nk, _ = out.shape
    tiles = nk // T
    zs, ys, xs = (lax.axis_size("rows"), lax.axis_size("slabs"), lax.axis_size("cols"))
    z, y, x = (lax.axis_index("rows"), lax.axis_index("slabs"), lax.axis_index("cols"))
    core = x % 2
    far_x = (x + 2 * core - 1 + xs) % xs
    near_x = x + 1 - 2 * core
    far, near = (1 + (ni - 1) * core, ni - (ni - 1) * core)
    far_halo, near_halo = ((ni + 1) * core, (ni + 1) * (1 - core))
    z_up, z_down = ((z + 1) % zs, (z + zs - 1) % zs)
    y_up, y_down = ((y + 1) % ys, (y + ys - 1) % ys)
    body = pl.ds(1, nj)
    levels = (a, b, a)

    def local(src, dst, n):
        return pltpu.make_async_copy(src, dst, load_sem.at[n])

    def wait_for(tiles_landed, sem):
        depth = tiles if tiles_landed % (ni * tiles) == 0 else 1
        part = (pl.ds(0, tiles_landed // (ni * depth)), pl.ds(0, ni), pl.ds(0, depth * T))
        pltpu.make_async_copy(p_hbm.at[part], s.at[part], sem).wait()

    plane = nj * tiles
    near_tiles, y_tiles, z_tiles = (nj, nj * ni // T, ni)

    def rows_of(kc):
        return pl.ds(T + kc * T, T)

    loads = []
    for kc in ORDER:
        loads.append(local(
            p_hbm.at[:, far - 1, pl.ds(kc * T, T), :], a.at[body, far, rows_of(kc), :], 0
        ))
    loads.append(local(p_hbm.at[:, near - 1], a.at[body, near, pl.ds(T, nk), :], 1))
    loads.append(local(
        p_hbm.at[:, pl.ds(1, ni - 2)], a.at[body, pl.ds(2, ni - 2), pl.ds(T, nk), :], 1
    ))
    for n, kc in enumerate(ORDER):
        loads.append(local(
            e_hbm.at[:, :, pl.ds(kc * T, T), :], b.at[body, pl.ds(1, ni), rows_of(kc), :], n + 2
        ))
        loads.append(local(
            s_hbm.at[:, :, pl.ds(kc * T, T), :], s.at[:, :, pl.ds(kc * T, T), :], n + 2
        ))
    for copy in loads:
        copy.start()

    def remote(src, dst, send, recv, **where):
        return pltpu.make_async_remote_copy(
            src_ref=src, dst_ref=dst, send_sem=send, recv_sem=recv, device_id=where, device_id_type=MESH
        )

    def far_piece(t, kc, n, start, size):
        ref = levels[t]
        part = pl.ds(1 + start, size)
        return remote(
            ref.at[part, far, rows_of(kc), :],
            ref.at[part, (ni + 1) * (1 - core), rows_of(kc), :],
            face_send.at[t], far_recv.at[kc + n] if t == STEPS - 1 else face_recv.at[t, kc], cols=far_x,
        )

    def pieces_of(t, kc):
        if t < STEPS - 1 or kc != ORDER[-1]:
            return [(kc, 0, 0, nj)]
        starts = [0]
        for part in TAIL:
            starts.append(starts[-1] + nj // part)
        ids = [0] + [tiles - kc + n for n in range(len(TAIL) - 1)]
        return [(kc, n, a0, a1 - a0) for n, a0, a1 in zip(ids, starts, starts[1:])]

    def far_copies(t, kc):
        return [far_piece(t, *piece) for piece in pieces_of(t, kc)]

    def near_copy(t, kc):
        ref = levels[t]
        return remote(
            ref.at[body, near, rows_of(kc), :],
            ref.at[body, (ni + 1) * core, rows_of(kc), :],
            face_send.at[t], face_recv.at[t, kc], cols=near_x,
        )

    def z_copies(t, kc):
        ref = levels[t]
        cells = pl.ds(1, ni)
        return (
            remote(
                ref.at[nj, cells, rows_of(kc), :], ref.at[0, cells, rows_of(kc), :],
                face_send.at[t], face_recv.at[t, kc], rows=z_up,
            ),
            remote(
                ref.at[1, cells, rows_of(kc), :], ref.at[nj + 1, cells, rows_of(kc), :],
                face_send.at[t], face_recv.at[t, kc], rows=z_down,
            ),
        )

    def y_copy(t, kc):
        ref = levels[t]
        cells = pl.ds(1, ni)
        if kc == 0:
            return remote(
                ref.at[body, cells, pl.ds(T, 1), :], ref.at[body, cells, pl.ds(T + nk, 1), :],
                face_send.at[t], face_recv.at[t, tiles - 1], slabs=y_down,
            )
        return remote(
            ref.at[body, cells, pl.ds(T + nk - 1, 1), :], ref.at[body, cells, pl.ds(T - 1, 1), :],
            face_send.at[t], face_recv.at[t, 0], slabs=y_up,
        )

    def faces(t, kc):
        yield from far_copies(t, kc)
        yield near_copy(t, kc)
        yield from z_copies(t, kc)
        if kc in (0, tiles - 1):
            yield y_copy(t, kc)

    def wait_faces(t, kc):
        landed = near_tiles + 2 * z_tiles
        if t < STEPS - 1:
            landed += near_tiles
        if kc in (0, tiles - 1):
            landed += y_tiles
        wait_for(landed, face_recv.at[t, kc])

    def wait_faces_sent(t):
        wait_for(2 * plane + 2 * z_tiles * tiles + 2 * y_tiles, face_send.at[t])

    def stepped(now, before, j, i, kc):
        r = T + kc * T
        middle = now[j, i, pl.ds(r, T), :]
        total = now[j - 1, i, pl.ds(r, T), :] + now[j + 1, i, pl.ds(r, T), :]
        total = total + now[j, i - 1, pl.ds(r, T), :] + now[j, i + 1, pl.ds(r, T), :]
        total = total + now[j, i, pl.ds(r - 1, T), :] + now[j, i, pl.ds(r + 1, T), :]
        spread = total - 6.0 * middle
        earlier = before[j, i, pl.ds(r, T), :]
        return 2.0 * middle - earlier + s[j - 1, i - 1, pl.ds(kc * T, T), :] * spread

    barrier = pltpu.get_barrier_semaphore()
    peers = [dict(cols=far_x), dict(cols=near_x), dict(slabs=y_up), dict(slabs=y_down)]
    others = [dict(rows=(z + d) % zs) for d in (2, 1, 3)]
    first, later = (peers[:2] + others, peers[2:])
    even = y % 2 == 0
    for where in first:
        pl.semaphore_signal(barrier, inc=1, device_id=where, device_id_type=MESH)
    pl.semaphore_wait(barrier, jnp.where(even, len(first), len(first) + len(later)))
    for where in later:
        pl.semaphore_signal(barrier, inc=1, device_id=where, device_id_type=MESH)

    wait_for(plane, load_sem.at[0])
    for kc in ORDER:
        for copy in far_copies(0, kc):
            copy.start()
    wait_for((ni - 1) * plane, load_sem.at[1])
    for kc in ORDER:
        near_copy(0, kc).start()
    for kc in ORDER:
        for copy in z_copies(0, kc):
            copy.start()

    @pl.when(even)
    def _():
        pl.semaphore_wait(barrier, len(later))

    y_copy(0, tiles - 1).start()
    y_copy(0, 0).start()

    for t in range(STEPS - 1):
        now, before = (levels[t], levels[(t + 1) % 2])
        if t > 0:
            wait_faces_sent(t - 1)
        for n, kc in enumerate(ORDER):
            if t == 0:
                wait_for(2 * ni * nj, load_sem.at[n + 2])
            wait_faces(t, kc)

            @pl.loop(0, nj // UNROLL)
            def _(g, now=now, before=before, kc=kc):
                for u in range(UNROLL):
                    j = 1 + g * UNROLL + u
                    for i in range(1, ni + 1):
                        before[j, i, pl.ds(T + kc * T, T), :] = stepped(now, before, j, i, kc)

            for copy in faces(t + 1, kc):
                copy.start()

    t = STEPS - 1
    now, before = (levels[t], levels[t - 1])
    inner = [near] + [i for i in range(2, ni)]

    def last_step(planes, kc, start, size, sums):
        def loop(g, sums):
            sums = list(sums)
            for u in range(UNROLL):
                j = 1 + start + g * UNROLL + u
                for n, i in enumerate(planes):
                    value = stepped(now, before, j, i, kc)
                    out[j - 1, i - 1, pl.ds(kc * T, T), :] = value
                    moved = value - GUESS
                    sums[2 * n] = sums[2 * n] + moved
                    sums[2 * n + 1] = sums[2 * n + 1] + moved * moved
            return tuple(sums)

        if sums is None:
            sums = (jnp.zeros((T, out.shape[3]), jnp.float32),) * (2 * len(planes))
        return lax.fori_loop(0, size // UNROLL, loop, sums)

    def put_sums(slots, kc, sums):
        for n, slot in enumerate(slots):
            stats[z, slot, 0, pl.ds(kc * T, T), :] = sums[2 * n]
            stats[z, slot, 1, pl.ds(kc * T, T), :] = sums[2 * n + 1]

    def send_sums(part, group):
        for where in others:
            remote(part, part, sums_send, sums_recv.at[group], **where).start()

    def finish(i, slot, kc):
        totals = stats[0, slot, 0, pl.ds(kc * T, T), :]
        squares = stats[0, slot, 1, pl.ds(kc * T, T), :]
        for other in range(1, zs):
            totals = totals + stats[other, slot, 0, pl.ds(kc * T, T), :]
            squares = squares + stats[other, slot, 1, pl.ds(kc * T, T), :]
        count = nj * zs
        shift = totals * (1.0 / count)
        variance = squares * (1.0 / count) - shift * shift
        norm[0, i - 1, pl.ds(kc * T, T), :] = GUESS + shift
        norm[1, i - 1, pl.ds(kc * T, T), :] = lax.rsqrt(variance + 0.0001)

    for kc in ORDER:
        wait_faces(t, kc)
        put_sums(range(1, ni), kc, last_step(inner, kc, 0, nj, None))
    send_sums(stats.at[z, pl.ds(1, ni - 1)], 0)
    wait_faces_sent(t - 1)
    peers_sums = 2 * len(others)
    for n, kc in enumerate(ORDER):
        sums = None
        for piece, copy in zip(pieces_of(t, kc), far_copies(t, kc)):
            copy.wait_recv()
            sums = last_step([far], kc, piece[2], piece[3], sums)
        put_sums([0], kc, sums)
        send_sums(stats.at[z, 0, :, pl.ds(kc * T, T), :], n // 2)
        if n == 2:
            wait_for(peers_sums * ((ni - 1) * tiles + 2), sums_recv.at[0])
            for slot, i in enumerate(inner):
                for tile in ORDER:
                    finish(i, slot + 1, tile)
            for tile in ORDER[:2]:
                finish(far, 0, tile)
    wait_for(peers_sums * 2, sums_recv.at[1])
    for tile in ORDER[2:]:
        finish(far, 0, tile)
    wait_faces_sent(t)
    wait_for(peers_sums * ni * tiles, sums_send)


def write_kernel(pieces, p, norm, scaled_hbm, end_hbm, scaled, scaled_sem, end_sem):
    nj, ni, nk, _ = p.shape
    step = nj // pieces

    def end(n):
        part = pl.ds(n * step, step)
        return pltpu.make_async_copy(p.at[part], end_hbm.at[part], end_sem)

    for n in range(pieces):
        end(n).start()

    def copy(n):
        part = pl.ds(n * step, step)
        return pltpu.make_async_copy(scaled.at[part], scaled_hbm.at[part], scaled_sem)

    for n in range(pieces):
        for i in range(ni):
            for kc in range(nk // T):
                rows = pl.ds(kc * T, T)
                mean, scale = (norm[0, i, rows, :], norm[1, i, rows, :])

                @pl.loop(n * step, (n + 1) * step, unroll=8)
                def _(j):
                    scaled[j, i, rows, :] = (p[j, i, rows, :] - mean) * scale

        copy(n).start()
    pltpu.make_async_copy(p, end_hbm, end_sem).wait()
    pltpu.make_async_copy(scaled, scaled_hbm, scaled_sem).wait()


def shards(pressure, earlier, speed_square):
    nj, ni, nk, members = pressure.shape
    tiles = nk // T
    zs = lax.axis_size("rows")
    whole = pl.BlockSpec(memory_space=pl.ANY)
    vmem = pl.BlockSpec(memory_space=pltpu.VMEM)
    f32 = jnp.float32
    dma = pltpu.SemaphoreType.DMA
    p, norm = pl.pallas_call(
        exchange_kernel,
        out_shape=(
            pltpu.VMEM((nj, ni, nk, members), f32),
            pltpu.VMEM((2, ni, nk, members), f32),
        ),
        in_specs=[whole] * 3,
        out_specs=(vmem, vmem),
        scratch_shapes=[
            pltpu.VMEM((nj + 2, ni + 2, nk + 2 * T, members), f32),
            pltpu.VMEM((nj + 2, ni + 2, nk + 2 * T, members), f32),
            pltpu.VMEM((nj, ni, nk, members), f32),
            pltpu.VMEM((zs, ni, 2, nk, members), f32),
            dma((tiles + 2,)),
            dma((STEPS,)), dma((STEPS, tiles)), dma((tiles + len(TAIL) - 1,)),
            dma, dma((2,)),
        ],
        compiler_params=pltpu.CompilerParams(
            collective_id=0, has_side_effects=True, vmem_limit_bytes=50 << 20
        ),
        name="leapfrog",
    )(pressure, earlier, speed_square)
    return pl.pallas_call(
        functools.partial(write_kernel, 8),
        out_shape=(jax.ShapeDtypeStruct(p.shape, f32),) * 2,
        in_specs=[vmem, vmem],
        out_specs=(whole, whole),
        scratch_shapes=[pltpu.VMEM(p.shape, f32), dma, dma],
        compiler_params=pltpu.CompilerParams(vmem_limit_bytes=20 << 20),
        name="centre_and_scale",
    )(p, norm)


def solution(mesh):
    spec = P("rows", "cols", "slabs", None)
    return jax.shard_map(shards, mesh=mesh, in_specs=(spec,) * 3, out_specs=(spec,) * 2, check_vma=False)
```

```python
import functools

import jax
import jax.numpy as jnp
from jax import lax
from jax.experimental import pallas as pl
from jax.experimental.pallas import tpu as pltpu
from jax.sharding import PartitionSpec as P

STEPS = 3
MESH = pl.DeviceIdType.MESH
T = 8
ORDER = (3, 0, 1, 2)
TAIL = (2, 4, 8, 8)
UNROLL = 2


def exchange_kernel(
    p_hbm, e_hbm, s_hbm, out, norm,
    a, b, s, stats,
    load_sem, face_send, face_recv, far_recv, sums_send, sums_recv,
):
    nj, ni, nk, _ = out.shape
    tiles = nk // T
    zs, ys, xs = (lax.axis_size("rows"), lax.axis_size("slabs"), lax.axis_size("cols"))
    z, y, x = (lax.axis_index("rows"), lax.axis_index("slabs"), lax.axis_index("cols"))
    core = x % 2
    far_x = (x + 2 * core - 1 + xs) % xs
    near_x = x + 1 - 2 * core
    far, near = (1 + (ni - 1) * core, ni - (ni - 1) * core)
    far_halo, near_halo = ((ni + 1) * core, (ni + 1) * (1 - core))
    z_up, z_down = ((z + 1) % zs, (z + zs - 1) % zs)
    y_up, y_down = ((y + 1) % ys, (y + ys - 1) % ys)
    body = pl.ds(1, nj)
    levels = (a, b, a)

    def local(src, dst, n):
        return pltpu.make_async_copy(src, dst, load_sem.at[n])

    def wait_for(tiles_landed, sem):
        depth = tiles if tiles_landed % (ni * tiles) == 0 else 1
        part = (pl.ds(0, tiles_landed // (ni * depth)), pl.ds(0, ni), pl.ds(0, depth * T))
        pltpu.make_async_copy(p_hbm.at[part], s.at[part], sem).wait()

    plane = nj * tiles
    near_tiles, y_tiles, z_tiles = (nj, nj * ni // T, ni)

    def rows_of(kc):
        return pl.ds(T + kc * T, T)

    loads = []
    for kc in ORDER:
        loads.append(local(
            p_hbm.at[:, far - 1, pl.ds(kc * T, T), :], a.at[body, far, rows_of(kc), :], 0
        ))
    loads.append(local(p_hbm.at[:, near - 1], a.at[body, near, pl.ds(T, nk), :], 1))
    loads.append(local(
        p_hbm.at[:, pl.ds(1, ni - 2)], a.at[body, pl.ds(2, ni - 2), pl.ds(T, nk), :], 1
    ))
    for n, kc in enumerate(ORDER):
        loads.append(local(
            e_hbm.at[:, :, pl.ds(kc * T, T), :], b.at[body, pl.ds(1, ni), rows_of(kc), :], n + 2
        ))
        loads.append(local(
            s_hbm.at[:, :, pl.ds(kc * T, T), :], s.at[:, :, pl.ds(kc * T, T), :], n + 2
        ))
    for copy in loads:
        copy.start()

    def remote(src, dst, send, recv, **where):
        return pltpu.make_async_remote_copy(
            src_ref=src, dst_ref=dst, send_sem=send, recv_sem=recv, device_id=where, device_id_type=MESH
        )

    def far_piece(t, kc, n, start, size):
        ref = levels[t]
        part = pl.ds(1 + start, size)
        return remote(
            ref.at[part, far, rows_of(kc), :],
            ref.at[part, (ni + 1) * (1 - core), rows_of(kc), :],
            face_send.at[t], far_recv.at[kc + n] if t == STEPS - 1 else face_recv.at[t, kc], cols=far_x,
        )

    def pieces_of(t, kc):
        if t < STEPS - 1 or kc != ORDER[-1]:
            return [(kc, 0, 0, nj)]
        starts = [0]
        for part in TAIL:
            starts.append(starts[-1] + nj // part)
        ids = [0] + [tiles - kc + n for n in range(len(TAIL) - 1)]
        return [(kc, n, a0, a1 - a0) for n, a0, a1 in zip(ids, starts, starts[1:])]

    def far_copies(t, kc):
        return [far_piece(t, *piece) for piece in pieces_of(t, kc)]

    def near_copy(t, kc):
        ref = levels[t]
        return remote(
            ref.at[body, near, rows_of(kc), :],
            ref.at[body, (ni + 1) * core, rows_of(kc), :],
            face_send.at[t], face_recv.at[t, kc], cols=near_x,
        )

    def z_copies(t, kc):
        ref = levels[t]
        cells = pl.ds(1, ni)
        return (
            remote(
                ref.at[nj, cells, rows_of(kc), :], ref.at[0, cells, rows_of(kc), :],
                face_send.at[t], face_recv.at[t, kc], rows=z_up,
            ),
            remote(
                ref.at[1, cells, rows_of(kc), :], ref.at[nj + 1, cells, rows_of(kc), :],
                face_send.at[t], face_recv.at[t, kc], rows=z_down,
            ),
        )

    def y_copy(t, kc):
        ref = levels[t]
        cells = pl.ds(1, ni)
        if kc == 0:
            return remote(
                ref.at[body, cells, pl.ds(T, 1), :], ref.at[body, cells, pl.ds(T + nk, 1), :],
                face_send.at[t], face_recv.at[t, tiles - 1], slabs=y_down,
            )
        return remote(
            ref.at[body, cells, pl.ds(T + nk - 1, 1), :], ref.at[body, cells, pl.ds(T - 1, 1), :],
            face_send.at[t], face_recv.at[t, 0], slabs=y_up,
        )

    def faces(t, kc):
        yield from far_copies(t, kc)
        yield near_copy(t, kc)
        yield from z_copies(t, kc)
        if kc in (0, tiles - 1):
            yield y_copy(t, kc)

    def wait_faces(t, kc):
        landed = near_tiles + 2 * z_tiles
        if t < STEPS - 1:
            landed += near_tiles
        if kc in (0, tiles - 1):
            landed += y_tiles
        wait_for(landed, face_recv.at[t, kc])

    def wait_faces_sent(t):
        wait_for(2 * plane + 2 * z_tiles * tiles + 2 * y_tiles, face_send.at[t])

    def stepped(now, before, j, i, kc):
        r = T + kc * T
        middle = now[j, i, pl.ds(r, T), :]
        total = now[j - 1, i, pl.ds(r, T), :] + now[j + 1, i, pl.ds(r, T), :]
        total = total + now[j, i - 1, pl.ds(r, T), :] + now[j, i + 1, pl.ds(r, T), :]
        total = total + now[j, i, pl.ds(r - 1, T), :] + now[j, i, pl.ds(r + 1, T), :]
        spread = total - 6.0 * middle
        earlier = before[j, i, pl.ds(r, T), :]
        return 2.0 * middle - earlier + s[j - 1, i - 1, pl.ds(kc * T, T), :] * spread

    barrier = pltpu.get_barrier_semaphore()
    peers = [dict(cols=far_x), dict(cols=near_x), dict(slabs=y_up), dict(slabs=y_down)]
    others = [dict(rows=(z + d) % zs) for d in (1, 3, 2)]
    first, later = (peers[:2] + others, peers[2:])
    even = y % 2 == 0
    for where in first:
        pl.semaphore_signal(barrier, inc=1, device_id=where, device_id_type=MESH)
    pl.semaphore_wait(barrier, jnp.where(even, len(first), len(first) + len(later)))
    for where in later:
        pl.semaphore_signal(barrier, inc=1, device_id=where, device_id_type=MESH)

    wait_for(plane, load_sem.at[0])
    for kc in ORDER:
        for copy in far_copies(0, kc):
            copy.start()
    wait_for((ni - 1) * plane, load_sem.at[1])
    for kc in ORDER:
        near_copy(0, kc).start()
    for kc in ORDER:
        for copy in z_copies(0, kc):
            copy.start()

    @pl.when(even)
    def _():
        pl.semaphore_wait(barrier, len(later))

    y_copy(0, tiles - 1).start()
    y_copy(0, 0).start()

    for t in range(STEPS - 1):
        now, before = (levels[t], levels[(t + 1) % 2])
        if t > 0:
            wait_faces_sent(t - 1)
        for n, kc in enumerate(ORDER):
            if t == 0:
                wait_for(2 * ni * nj, load_sem.at[n + 2])
            wait_faces(t, kc)

            @pl.loop(0, nj // UNROLL)
            def _(g, now=now, before=before, kc=kc):
                for u in range(UNROLL):
                    j = 1 + g * UNROLL + u
                    for i in range(1, ni + 1):
                        before[j, i, pl.ds(T + kc * T, T), :] = stepped(now, before, j, i, kc)

            for copy in faces(t + 1, kc):
                copy.start()

    t = STEPS - 1
    now, before = (levels[t], levels[t - 1])
    inner = [near] + [i for i in range(2, ni)]

    def guess(i, kc):
        row = (1, i, pl.ds(T + kc * T, T))
        return 2.0 * now[row] - before[row]

    def last_step(planes, kc, start, size, sums):
        guesses = [guess(i, kc) for i in planes]

        def loop(g, sums):
            sums = list(sums)
            for u in range(UNROLL):
                j = 1 + start + g * UNROLL + u
                for n, i in enumerate(planes):
                    value = stepped(now, before, j, i, kc)
                    out[j - 1, i - 1, pl.ds(kc * T, T), :] = value
                    moved = value - guesses[n]
                    sums[2 * n] = sums[2 * n] + moved
                    sums[2 * n + 1] = sums[2 * n + 1] + moved * moved
            return tuple(sums)

        if sums is None:
            sums = (jnp.zeros((T, out.shape[3]), jnp.float32),) * (2 * len(planes))
        return lax.fori_loop(0, size // UNROLL, loop, sums)

    def put_sums(planes, slots, kc, sums):
        for n, (i, slot) in enumerate(zip(planes, slots)):
            shift = sums[2 * n] * (1.0 / nj)
            stats[z, slot, 0, pl.ds(kc * T, T), :] = guess(i, kc) + shift
            stats[z, slot, 1, pl.ds(kc * T, T), :] = sums[2 * n + 1] - sums[2 * n] * shift

    def send_sums(part, group):
        for where in others:
            remote(part, part, sums_send, sums_recv.at[group], **where).start()

    def finish(i, slot, kc):
        means = [stats[other, slot, 0, pl.ds(kc * T, T), :] for other in range(zs)]
        squares = [stats[other, slot, 1, pl.ds(kc * T, T), :] for other in range(zs)]
        mean = sum(means[1:], means[0]) * (1.0 / zs)
        between = [(m - mean) * (m - mean) for m in means]
        variance = sum(squares[1:], squares[0]) * (1.0 / (nj * zs))
        variance = variance + sum(between[1:], between[0]) * (1.0 / zs)
        norm[0, i - 1, pl.ds(kc * T, T), :] = mean
        norm[1, i - 1, pl.ds(kc * T, T), :] = lax.rsqrt(variance + 0.0001)

    for kc in ORDER:
        wait_faces(t, kc)
        put_sums(inner, range(1, ni), kc, last_step(inner, kc, 0, nj, None))
    send_sums(stats.at[z, pl.ds(1, ni - 1)], 0)
    wait_faces_sent(t - 1)
    peers_sums = 2 * len(others)
    for n, kc in enumerate(ORDER):
        sums = None
        for piece, copy in zip(pieces_of(t, kc), far_copies(t, kc)):
            copy.wait_recv()
            sums = last_step([far], kc, piece[2], piece[3], sums)
        put_sums([far], [0], kc, sums)
        send_sums(stats.at[z, 0, :, pl.ds(kc * T, T), :], n // 2)
        if n == 2:
            wait_for(peers_sums * ((ni - 1) * tiles + 2), sums_recv.at[0])
            for slot, i in enumerate(inner):
                for tile in ORDER:
                    finish(i, slot + 1, tile)
            for tile in ORDER[:2]:
                finish(far, 0, tile)
    wait_for(peers_sums * 2, sums_recv.at[1])
    for tile in ORDER[2:]:
        finish(far, 0, tile)
    wait_faces_sent(t)
    wait_for(peers_sums * ni * tiles, sums_send)


def write_kernel(pieces, p, norm, scaled_hbm, end_hbm, scaled, scaled_sem, end_sem):
    nj, ni, nk, _ = p.shape
    step = nj // pieces

    def end(n):
        part = pl.ds(n * step, step)
        return pltpu.make_async_copy(p.at[part], end_hbm.at[part], end_sem)

    for n in range(pieces):
        end(n).start()

    def copy(n):
        part = pl.ds(n * step, step)
        return pltpu.make_async_copy(scaled.at[part], scaled_hbm.at[part], scaled_sem)

    for n in range(pieces):

        @pl.loop(n * step, (n + 1) * step, unroll=2)
        def _(j):
            for i in range(ni):
                scaled[j, i] = (p[j, i] - norm[0, i]) * norm[1, i]

        copy(n).start()
    pltpu.make_async_copy(p, end_hbm, end_sem).wait()
    pltpu.make_async_copy(scaled, scaled_hbm, scaled_sem).wait()


def shards(pressure, earlier, speed_square):
    nj, ni, nk, members = pressure.shape
    tiles = nk // T
    zs = lax.axis_size("rows")
    whole = pl.BlockSpec(memory_space=pl.ANY)
    vmem = pl.BlockSpec(memory_space=pltpu.VMEM)
    f32 = jnp.float32
    dma = pltpu.SemaphoreType.DMA
    p, norm = pl.pallas_call(
        exchange_kernel,
        out_shape=(
            pltpu.VMEM((nj, ni, nk, members), f32),
            pltpu.VMEM((2, ni, nk, members), f32),
        ),
        in_specs=[whole] * 3,
        out_specs=(vmem, vmem),
        scratch_shapes=[
            pltpu.VMEM((nj + 2, ni + 2, nk + 2 * T, members), f32),
            pltpu.VMEM((nj + 2, ni + 2, nk + 2 * T, members), f32),
            pltpu.VMEM((nj, ni, nk, members), f32),
            pltpu.VMEM((zs, ni, 2, nk, members), f32),
            dma((tiles + 2,)),
            dma((STEPS,)), dma((STEPS, tiles)), dma((tiles + len(TAIL) - 1,)),
            dma, dma((2,)),
        ],
        compiler_params=pltpu.CompilerParams(
            collective_id=0, has_side_effects=True, vmem_limit_bytes=50 << 20
        ),
        name="leapfrog",
    )(pressure, earlier, speed_square)
    return pl.pallas_call(
        functools.partial(write_kernel, 8),
        out_shape=(jax.ShapeDtypeStruct(p.shape, f32),) * 2,
        in_specs=[vmem, vmem],
        out_specs=(whole, whole),
        scratch_shapes=[pltpu.VMEM(p.shape, f32), dma, dma],
        compiler_params=pltpu.CompilerParams(vmem_limit_bytes=20 << 20),
        name="centre_and_scale",
    )(p, norm)


def solution(mesh):
    spec = P("rows", "cols", "slabs", None)
    return jax.shard_map(shards, mesh=mesh, in_specs=(spec,) * 3, out_specs=(spec,) * 2, check_vma=False)
```

```python
import functools

import jax
import jax.numpy as jnp
from jax import lax
from jax.experimental import pallas as pl
from jax.experimental.pallas import tpu as pltpu
from jax.sharding import PartitionSpec as P

STEPS = 3
MESH = pl.DeviceIdType.MESH
T = 8
ORDER = (3, 0, 1, 2)
TAIL = (2, 4, 8, 8)
UNROLL = 2


def exchange_kernel(
    p_hbm, e_hbm, s_hbm, out, norm,
    a, b, s, stats,
    load_sem, face_send, face_recv, far_recv, sums_send, sums_recv,
):
    nj, ni, nk, _ = out.shape
    tiles = nk // T
    zs, ys, xs = (lax.axis_size("rows"), lax.axis_size("slabs"), lax.axis_size("cols"))
    z, y, x = (lax.axis_index("rows"), lax.axis_index("slabs"), lax.axis_index("cols"))
    core = x % 2
    far_x = (x + 2 * core - 1 + xs) % xs
    near_x = x + 1 - 2 * core
    far, near = (1 + (ni - 1) * core, ni - (ni - 1) * core)
    far_halo, near_halo = ((ni + 1) * core, (ni + 1) * (1 - core))
    z_up, z_down = ((z + 1) % zs, (z + zs - 1) % zs)
    y_up, y_down = ((y + 1) % ys, (y + ys - 1) % ys)
    body = pl.ds(1, nj)
    levels = (a, b, a)

    def local(src, dst, n):
        return pltpu.make_async_copy(src, dst, load_sem.at[n])

    def wait_for(tiles_landed, sem):
        depth = tiles if tiles_landed % (ni * tiles) == 0 else 1
        part = (pl.ds(0, tiles_landed // (ni * depth)), pl.ds(0, ni), pl.ds(0, depth * T))
        pltpu.make_async_copy(p_hbm.at[part], s.at[part], sem).wait()

    plane = nj * tiles
    near_tiles, y_tiles, z_tiles = (nj, nj * ni // T, ni)

    def rows_of(kc):
        return pl.ds(T + kc * T, T)

    loads = []
    for kc in ORDER:
        loads.append(local(
            p_hbm.at[:, far - 1, pl.ds(kc * T, T), :], a.at[body, far, rows_of(kc), :], 0
        ))
    loads.append(local(p_hbm.at[:, near - 1], a.at[body, near, pl.ds(T, nk), :], 1))
    loads.append(local(
        p_hbm.at[:, pl.ds(1, ni - 2)], a.at[body, pl.ds(2, ni - 2), pl.ds(T, nk), :], 1
    ))
    for n, kc in enumerate(ORDER):
        loads.append(local(
            e_hbm.at[:, :, pl.ds(kc * T, T), :], b.at[body, pl.ds(1, ni), rows_of(kc), :], n // 2 + 2
        ))
        loads.append(local(
            s_hbm.at[:, :, pl.ds(kc * T, T), :], s.at[:, :, pl.ds(kc * T, T), :], n // 2 + 2
        ))
    for copy in loads:
        copy.start()

    def remote(src, dst, send, recv, **where):
        return pltpu.make_async_remote_copy(
            src_ref=src, dst_ref=dst, send_sem=send, recv_sem=recv, device_id=where, device_id_type=MESH
        )

    def far_piece(t, kc, n, start, size):
        ref = levels[t]
        part = pl.ds(1 + start, size)
        return remote(
            ref.at[part, far, rows_of(kc), :],
            ref.at[part, (ni + 1) * (1 - core), rows_of(kc), :],
            face_send.at[t % 2], far_recv.at[kc + n] if t == STEPS - 1 else face_recv.at[t % 2, kc], cols=far_x,
        )

    def pieces_of(t, kc):
        if t < STEPS - 1 or kc != ORDER[-1]:
            return [(kc, 0, 0, nj)]
        starts = [0]
        for part in TAIL:
            starts.append(starts[-1] + nj // part)
        ids = [0] + [tiles - kc + n for n in range(len(TAIL) - 1)]
        return [(kc, n, a0, a1 - a0) for n, a0, a1 in zip(ids, starts, starts[1:])]

    def far_copies(t, kc):
        return [far_piece(t, *piece) for piece in pieces_of(t, kc)]

    def near_copy(t, kc):
        ref = levels[t]
        return remote(
            ref.at[body, near, rows_of(kc), :],
            ref.at[body, (ni + 1) * core, rows_of(kc), :],
            face_send.at[t % 2], face_recv.at[t % 2, kc], cols=near_x,
        )

    def z_copies(t, kc):
        ref = levels[t]
        cells = pl.ds(1, ni)
        return (
            remote(
                ref.at[nj, cells, rows_of(kc), :], ref.at[0, cells, rows_of(kc), :],
                face_send.at[t % 2], face_recv.at[t % 2, kc], rows=z_up,
            ),
            remote(
                ref.at[1, cells, rows_of(kc), :], ref.at[nj + 1, cells, rows_of(kc), :],
                face_send.at[t % 2], face_recv.at[t % 2, kc], rows=z_down,
            ),
        )

    def y_copy(t, kc):
        ref = levels[t]
        cells = pl.ds(1, ni)
        if kc == 0:
            return remote(
                ref.at[body, cells, pl.ds(T, 1), :], ref.at[body, cells, pl.ds(T + nk, 1), :],
                face_send.at[t % 2], face_recv.at[t % 2, tiles - 1], slabs=y_down,
            )
        return remote(
            ref.at[body, cells, pl.ds(T + nk - 1, 1), :], ref.at[body, cells, pl.ds(T - 1, 1), :],
            face_send.at[t % 2], face_recv.at[t % 2, 0], slabs=y_up,
        )

    def faces(t, kc):
        yield from far_copies(t, kc)
        yield near_copy(t, kc)
        yield from z_copies(t, kc)
        if kc in (0, tiles - 1):
            yield y_copy(t, kc)

    def wait_faces(t, kc):
        landed = near_tiles + 2 * z_tiles
        if t < STEPS - 1:
            landed += near_tiles
        if kc in (0, tiles - 1):
            landed += y_tiles
        wait_for(landed, face_recv.at[t % 2, kc])

    def wait_faces_sent(t):
        wait_for(2 * plane + 2 * z_tiles * tiles + 2 * y_tiles, face_send.at[t % 2])

    def stepped(now, before, j, i, kc):
        r = T + kc * T
        middle = now[j, i, pl.ds(r, T), :]
        total = now[j - 1, i, pl.ds(r, T), :] + now[j + 1, i, pl.ds(r, T), :]
        total = total + now[j, i - 1, pl.ds(r, T), :] + now[j, i + 1, pl.ds(r, T), :]
        total = total + now[j, i, pl.ds(r - 1, T), :] + now[j, i, pl.ds(r + 1, T), :]
        spread = total - 6.0 * middle
        earlier = before[j, i, pl.ds(r, T), :]
        return 2.0 * middle - earlier + s[j - 1, i - 1, pl.ds(kc * T, T), :] * spread

    barrier = pltpu.get_barrier_semaphore()
    peers = [dict(cols=far_x), dict(cols=near_x), dict(slabs=y_up), dict(slabs=y_down)]
    others = [dict(rows=(z + d) % zs) for d in (1, 3, 2)]
    first, later = (peers[:2] + others, peers[2:])
    even = y % 2 == 0
    for where in first:
        pl.semaphore_signal(barrier, inc=1, device_id=where, device_id_type=MESH)
    pl.semaphore_wait(barrier, jnp.where(even, len(first), len(first) + len(later)))
    for where in later:
        pl.semaphore_signal(barrier, inc=1, device_id=where, device_id_type=MESH)

    wait_for(plane, load_sem.at[0])
    for kc in ORDER:
        for copy in far_copies(0, kc):
            copy.start()
    wait_for((ni - 1) * plane, load_sem.at[1])
    for kc in ORDER:
        near_copy(0, kc).start()
    for kc in ORDER:
        for copy in z_copies(0, kc):
            copy.start()

    @pl.when(even)
    def _():
        pl.semaphore_wait(barrier, len(later))

    y_copy(0, tiles - 1).start()
    y_copy(0, 0).start()

    for t in range(STEPS - 1):
        now, before = (levels[t], levels[(t + 1) % 2])
        if t > 0:
            wait_faces_sent(t - 1)
        for n, kc in enumerate(ORDER):
            if t == 0 and n % 2 == 0:
                wait_for(4 * ni * nj, load_sem.at[n // 2 + 2])
            wait_faces(t, kc)

            @pl.loop(0, nj // UNROLL)
            def _(g, now=now, before=before, kc=kc):
                for u in range(UNROLL):
                    j = 1 + g * UNROLL + u
                    for i in range(1, ni + 1):
                        before[j, i, pl.ds(T + kc * T, T), :] = stepped(now, before, j, i, kc)

            for copy in faces(t + 1, kc):
                copy.start()

    t = STEPS - 1
    now, before = (levels[t], levels[t - 1])
    inner = [near] + [i for i in range(2, ni)]

    def guess(i, kc):
        row = (1, i, pl.ds(T + kc * T, T))
        return 2.0 * now[row] - before[row]

    def last_step(planes, kc, start, size, sums):
        guesses = [guess(i, kc) for i in planes]

        def loop(g, sums):
            sums = list(sums)
            for u in range(UNROLL):
                j = 1 + start + g * UNROLL + u
                for n, i in enumerate(planes):
                    value = stepped(now, before, j, i, kc)
                    out[j - 1, i - 1, pl.ds(kc * T, T), :] = value
                    moved = value - guesses[n]
                    sums[2 * n] = sums[2 * n] + moved
                    sums[2 * n + 1] = sums[2 * n + 1] + moved * moved
            return tuple(sums)

        if sums is None:
            sums = (jnp.zeros((T, out.shape[3]), jnp.float32),) * (2 * len(planes))
        return lax.fori_loop(0, size // UNROLL, loop, sums)

    def put_sums(planes, slots, kc, sums):
        for n, (i, slot) in enumerate(zip(planes, slots)):
            shift = sums[2 * n] * (1.0 / nj)
            stats[z, slot, 0, pl.ds(kc * T, T), :] = guess(i, kc) + shift
            stats[z, slot, 1, pl.ds(kc * T, T), :] = sums[2 * n + 1] - sums[2 * n] * shift

    def send_sums(part, group):
        for where in others:
            remote(part, part, sums_send, sums_recv.at[group], **where).start()

    def finish(i, slot, kc):
        means = [stats[other, slot, 0, pl.ds(kc * T, T), :] for other in range(zs)]
        squares = [stats[other, slot, 1, pl.ds(kc * T, T), :] for other in range(zs)]
        mean = sum(means[1:], means[0]) * (1.0 / zs)
        between = [(m - mean) * (m - mean) for m in means]
        variance = sum(squares[1:], squares[0]) * (1.0 / (nj * zs))
        variance = variance + sum(between[1:], between[0]) * (1.0 / zs)
        norm[0, i - 1, pl.ds(kc * T, T), :] = mean
        norm[1, i - 1, pl.ds(kc * T, T), :] = lax.rsqrt(variance + 0.0001)

    for kc in ORDER:
        wait_faces(t, kc)
        put_sums(inner, range(1, ni), kc, last_step(inner, kc, 0, nj, None))
    send_sums(stats.at[z, pl.ds(1, ni - 1)], 0)
    wait_faces_sent(t - 1)
    peers_sums = 2 * len(others)
    for n, kc in enumerate(ORDER):
        sums = None
        for piece, copy in zip(pieces_of(t, kc), far_copies(t, kc)):
            copy.wait_recv()
            sums = last_step([far], kc, piece[2], piece[3], sums)
        put_sums([far], [0], kc, sums)
        send_sums(stats.at[z, 0, :, pl.ds(kc * T, T), :], n // 2)
        if n == 2:
            wait_for(peers_sums * ((ni - 1) * tiles + 2), sums_recv.at[0])
            for slot, i in enumerate(inner):
                for tile in ORDER:
                    finish(i, slot + 1, tile)
            for tile in ORDER[:2]:
                finish(far, 0, tile)
    wait_for(peers_sums * 2, sums_recv.at[1])
    for tile in ORDER[2:]:
        finish(far, 0, tile)
    wait_faces_sent(t)
    wait_for(peers_sums * ni * tiles, sums_send)


def write_kernel(pieces, p, norm, scaled_hbm, end_hbm, scaled, scaled_sem, end_sem):
    nj, ni, nk, _ = p.shape
    step = nj // pieces

    def end(n):
        part = pl.ds(n * step, step)
        return pltpu.make_async_copy(p.at[part], end_hbm.at[part], end_sem)

    for n in range(pieces):
        end(n).start()

    def copy(n):
        part = pl.ds(n * step, step)
        return pltpu.make_async_copy(scaled.at[part], scaled_hbm.at[part], scaled_sem)

    for n in range(pieces):

        @pl.loop(n * step, (n + 1) * step, unroll=2)
        def _(j):
            for i in range(ni):
                scaled[j, i] = (p[j, i] - norm[0, i]) * norm[1, i]

        copy(n).start()
    pltpu.make_async_copy(p, end_hbm, end_sem).wait()
    pltpu.make_async_copy(scaled, scaled_hbm, scaled_sem).wait()


def shards(pressure, earlier, speed_square):
    nj, ni, nk, members = pressure.shape
    tiles = nk // T
    zs = lax.axis_size("rows")
    whole = pl.BlockSpec(memory_space=pl.ANY)
    vmem = pl.BlockSpec(memory_space=pltpu.VMEM)
    f32 = jnp.float32
    dma = pltpu.SemaphoreType.DMA
    p, norm = pl.pallas_call(
        exchange_kernel,
        out_shape=(
            pltpu.VMEM((nj, ni, nk, members), f32),
            pltpu.VMEM((2, ni, nk, members), f32),
        ),
        in_specs=[whole] * 3,
        out_specs=(vmem, vmem),
        scratch_shapes=[
            pltpu.VMEM((nj + 2, ni + 2, nk + 2 * T, members), f32),
            pltpu.VMEM((nj + 2, ni + 2, nk + 2 * T, members), f32),
            pltpu.VMEM((nj, ni, nk, members), f32),
            pltpu.VMEM((zs, ni, 2, nk, members), f32),
            dma((tiles // 2 + 2,)),
            dma((2,)), dma((2, tiles)), dma((tiles + len(TAIL) - 1,)),
            dma, dma((2,)),
        ],
        compiler_params=pltpu.CompilerParams(
            collective_id=0, has_side_effects=True, vmem_limit_bytes=50 << 20
        ),
        name="leapfrog",
    )(pressure, earlier, speed_square)
    return pl.pallas_call(
        functools.partial(write_kernel, 8),
        out_shape=(jax.ShapeDtypeStruct(p.shape, f32),) * 2,
        in_specs=[vmem, vmem],
        out_specs=(whole, whole),
        scratch_shapes=[pltpu.VMEM(p.shape, f32), dma, dma],
        compiler_params=pltpu.CompilerParams(vmem_limit_bytes=20 << 20),
        name="centre_and_scale",
    )(p, norm)


def solution(mesh):
    spec = P("rows", "cols", "slabs", None)
    return jax.shard_map(shards, mesh=mesh, in_specs=(spec,) * 3, out_specs=(spec,) * 2, check_vma=False)
```
